32 devices in a mesh: row: 8 (over y, x, core), col: 4 (over z).
Axes of the slice: x: 2, y: 2, z: 4, core: 2. Of those that a mesh axis runs over, the one named last changes fastest.
Arguments:
- features: bfloat16 [32768, 512], P('col', 'row'), may hold values from -6 to 6
- weight_t: bfloat16 [512, 512], P(None, 'row'), may hold values from -0.25 to 0.25
- tiles: bfloat16 [8192, 128, 128], P(('row', 'col')), may hold values from -0.15625 to 0.15625
- coords: int32 [2, 8192], P(None, ('row', 'col')), may hold values from 0 to 63, as said below
- counts: int32 [32], P(('row', 'col')), may hold values from 32 to 256, as said below
Outputs:
- output: bfloat16 [32768, 512], P('row', 'col')
The draws below stay inside these ranges and needn't reach their ends.
Inputs may be any that keep to these rules, and one draw needn't show every extreme that they name: coords[0] of a slot lies in 0 to 31 and coords[1] in 0 to 63; the live slots of one grid cell name distinct tiles. `counts`: some grid cell has all 256 slots live in every draw.
All inputs are finite; a program needn't handle non-finite values.
Results may differ from the reference program's by a relative error of at most 0.0095.
Values may be sent and summed in bfloat16 or wider, within the bound.
A program may use at most 128 MiB of HBM per device.

```python
import jax
import jax.numpy as jnp
from jax import lax

TILE = 128
FEAT = 512
F_OUT = 512
TROW = 32
MAXT = 256
TCOL = 64
NODES = 32768
N_COL = 4
DEVICES = 32


def draw_coords(key, part):
    keys = jax.random.split(jax.random.fold_in(key, 11), DEVICES)
    spots = jax.vmap(lambda k: jax.random.permutation(k, TROW * TCOL)[:MAXT])(keys)
    spots = spots.reshape(DEVICES * MAXT).astype(jnp.int32)
    return jnp.stack([spots // TCOL, spots % TCOL]).astype(jnp.int32)


def draw_counts(key, part):
    base = jax.random.randint(jax.random.fold_in(key, 21), (DEVICES,), MAXT // 8, MAXT // 2 + 1)
    heavy = jax.random.randint(jax.random.fold_in(key, 22), (DEVICES,), 0, 8) == 0
    chosen = jax.random.randint(jax.random.fold_in(key, 23), (), 0, DEVICES)
    heavy = heavy | (jnp.arange(DEVICES, dtype=jnp.int32) == chosen)
    return jnp.where(heavy, MAXT, base).astype(jnp.int32)


def level_of(key, shape, cuts, least, high):
    level, own = 1.0, jax.random.fold_in(key, 6)
    for axis_at, parts in cuts:
        heights = jnp.exp(jax.random.uniform(jax.random.fold_in(own, axis_at), (parts,), jnp.float32, least / len(cuts), high / len(cuts)))
        level = level * jnp.repeat(heights, shape[axis_at] // parts).reshape([-1 if axis == axis_at else 1 for axis in range(len(shape))])
    return level


def scatter_about(key, dims, deviation, limit, pieces=(), kind=jnp.bfloat16):
    values = deviation * jax.random.normal(key, dims, jnp.float32)
    if pieces:
        values = values * level_of(key, dims, pieces, -0.22, 0.18)
    return jnp.clip(values, -limit, limit).astype(kind)


def setup_inputs(seed: int = 0) -> dict:
    streams_of = jax.random.split(jax.random.key(seed), 6)
    return {
        "features": scatter_about(streams_of[0], (NODES, FEAT), 1.0, 6.0, ((0, 4), (1, 8))),
        "weight_t": scatter_about(streams_of[1], (F_OUT, FEAT), FEAT ** -0.5, 0.25, ((1, 8),)),
        "tiles": scatter_about(streams_of[2], (DEVICES * MAXT, TILE, TILE), (2 * MAXT * TILE * N_COL // (5 * TROW)) ** -0.5, 0.15625, ((0, 32),)),
        "coords": draw_coords(jax.random.fold_in(streams_of[5], 71), 0),
        "counts": draw_counts(jax.random.fold_in(streams_of[5], 71), 0),
    }


def reference(features, weight_t, tiles, coords, counts):
    feat = features.shape[1]
    cblock = TCOL * TILE
    rblock = TROW * TILE
    lanes = jnp.arange(TROW, dtype=jnp.int32)
    slots = jnp.arange(MAXT, dtype=jnp.int32)

    def device(total, cell):
        rpos = cell // N_COL
        cpos = cell % N_COL
        block = lax.dynamic_slice_in_dim(tiles, (cell * MAXT).astype(jnp.int32), MAXT, 0).astype(jnp.float32)
        place = lax.dynamic_slice_in_dim(coords, (cell * MAXT).astype(jnp.int32), MAXT, 1)
        live = (slots < counts[cell]).astype(jnp.float32)
        panel = lax.dynamic_slice_in_dim(features, (cpos * cblock).astype(jnp.int32), cblock, 0)
        panel = panel.astype(jnp.float32).reshape(TCOL, TILE, feat)
        picked = panel[place[1]]
        prod = jnp.einsum('gij,gjw->giw', block * live[:, None, None], picked, precision=lax.Precision.HIGHEST)
        select = (place[0][:, None] == lanes[None, :]).astype(jnp.float32)
        part = jnp.einsum('gt,giw->tiw', select, prod, precision=lax.Precision.HIGHEST).reshape(rblock, feat)
        start = (rpos * rblock).astype(jnp.int32)
        old = lax.dynamic_slice_in_dim(total, start, rblock, 0)
        return lax.dynamic_update_slice_in_dim(total, old + part, start, 0), None

    total = jnp.zeros((NODES, feat), jnp.float32)
    total, _ = lax.scan(device, total, jnp.arange(DEVICES, dtype=jnp.int32))
    result = jnp.dot(total, weight_t.astype(jnp.float32).T, precision=lax.Precision.HIGHEST)
    return result.astype(jnp.bfloat16)
```

```python
import functools

import jax
import jax.numpy as jnp
from jax import lax
from jax.experimental import pallas as pl
from jax.experimental.pallas import tpu as pltpu
from jax.sharding import PartitionSpec as P

TROW = 32
GATHER_PIECES = 8
REDUCE_PIECES = 8
GROUP = 32
VMEM_LIMIT = 62 * 1024 * 1024


def swapped(p):
    return p + ((p // 2) % 2) * (1 - 2 * (p % 2))


def remote(src, dst, send, recv, axis, to):
    return pltpu.make_async_remote_copy(
        src_ref=src,
        dst_ref=dst,
        send_sem=send,
        recv_sem=recv,
        device_id={axis: to},
        device_id_type=pl.DeviceIdType.MESH,
    )


def gather_kernel(pairs, f_ref, w_ref, panel_ref, half_f, half_w,
                  pre_send, pre_recv, send_sem, recv_sem, sib_send, sib_recv):
    me = lax.axis_index("row")
    core = me % 2
    place = swapped(me // 2)
    sibling = me + 1 - 2 * core
    right = 2 * swapped(lax.rem(place + 1, pairs)) + core
    left = 2 * swapped(lax.rem(place + pairs - 1, pairs)) + core
    nodes = half_f.shape[0]
    outs = half_w.shape[0]
    thick = (nodes + outs) // GATHER_PIECES
    width = f_ref.shape[1]
    half = GATHER_PIECES // 2

    barrier = pltpu.get_barrier_semaphore()
    for other in (sibling, right, left):
        pl.semaphore_signal(
            barrier, inc=1, device_id={"row": other}, device_id_type=pl.DeviceIdType.MESH
        )
    pl.semaphore_wait(barrier, 3)

    theirs = 1 - core
    pre = [
        remote(f_ref.at[pl.ds(pl.multiple_of(theirs * nodes, nodes), nodes)], half_f,
               pre_send.at[0], pre_recv.at[0], "row", sibling),
        remote(w_ref.at[pl.ds(pl.multiple_of(theirs * outs, outs), outs)], half_w,
               pre_send.at[1], pre_recv.at[1], "row", sibling),
    ]
    for copy in pre:
        copy.start()
    for copy in pre:
        copy.wait()
    pair = me // 2

    @pl.when(core == 0)
    def _():
        panel_ref[pair, 0, :nodes, :width] = f_ref[:nodes]
        panel_ref[pair, 0, :nodes, width:] = half_f[...]
        panel_ref[pair, 0, nodes:, :width] = w_ref[:outs]
        panel_ref[pair, 0, nodes:, width:] = half_w[...]

    @pl.when(core == 1)
    def _():
        panel_ref[pair, 1, :nodes, :width] = half_f[...]
        panel_ref[pair, 1, :nodes, width:] = f_ref[nodes:]
        panel_ref[pair, 1, nodes:, :width] = half_w[...]
        panel_ref[pair, 1, nodes:, width:] = w_ref[outs:]

    sends = []

    def piece(position, index):
        return panel_ref.at[swapped(position), core, pl.ds(index * thick, thick)]

    def along(way, distance, position, index, to):
        ref = piece(position, index)
        return remote(ref, ref, send_sem.at[way, distance, index],
                      recv_sem.at[way, distance, index], "row", to)

    sib_at = [0]

    def share(position, index):
        ref = piece(position, index)
        copy = remote(ref, ref, sib_send.at[sib_at[0]], sib_recv.at[sib_at[0]], "row", sibling)
        sib_at[0] += 1
        copy.start()
        sends.append(copy)

    longest = pairs // 2

    def carried(way, distance):
        indices = list(range(GATHER_PIECES)) if way == 0 else list(range(half, GATHER_PIECES)) + list(range(half))
        return indices if distance < longest else indices[:half]

    def start(way, distance, position, index):
        copy = along(way, distance, position, index, right if way == 0 else left)
        copy.start()
        return copy

    issued = []
    for i in range(GATHER_PIECES):
        for way in range(2):
            issued.append(start(way, 0, place, carried(way, 0)[i]))
    for i in range(GATHER_PIECES):
        share(place, i)
    for distance in range(1, longest + 1):
        from_left = lax.rem(place + pairs - distance, pairs)
        from_right = lax.rem(place + distance, pairs)
        for i in range(len(carried(0, distance))):
            for way, position in ((0, from_left), (1, from_right)):
                index = carried(way, distance)[i]
                along(way, distance - 1, position, index, right).wait_recv()
                if distance < longest and index in carried(way, distance + 1):
                    issued.append(start(way, distance, position, index))
                share(position, index)
    for copy in issued:
        copy.wait_send()
    for copy in sends:
        copy.wait()


def gather(features, weight_t, pairs):
    nodes, width = features.shape
    outs = weight_t.shape[0]
    rows = (nodes + outs) // 2
    longest = pairs // 2
    return pl.pallas_call(
        functools.partial(gather_kernel, pairs),
        out_shape=jax.ShapeDtypeStruct((pairs, 2, rows, 2 * width), features.dtype),
        in_specs=[pl.BlockSpec(memory_space=pltpu.VMEM)] * 2,
        out_specs=pl.BlockSpec(memory_space=pltpu.VMEM),
        scratch_shapes=[
            pltpu.VMEM((nodes // 2, width), features.dtype),
            pltpu.VMEM((outs // 2, width), features.dtype),
            pltpu.SemaphoreType.DMA((2,)),
            pltpu.SemaphoreType.DMA((2,)),
            pltpu.SemaphoreType.DMA((2, longest, GATHER_PIECES)),
            pltpu.SemaphoreType.DMA((2, longest, GATHER_PIECES)),
            pltpu.SemaphoreType.DMA((pairs * GATHER_PIECES,)),
            pltpu.SemaphoreType.DMA((pairs * GATHER_PIECES,)),
        ],
        compiler_params=pltpu.CompilerParams(
            collective_id=0, has_side_effects=True, vmem_limit_bytes=VMEM_LIMIT
        ),
        name="gather",
    )(features, weight_t)


def spread_kernel(nodes, coords_ref, counts_ref, panel_ref, tiles_ref, out_ref, total, weight):
    step = pl.program_id(0)
    group, tile, _ = tiles_ref.shape
    pairs = panel_ref.shape[0]
    here = nodes // tile
    count = counts_ref[0]

    @pl.when(step == 0)
    def _():
        total[...] = jnp.zeros_like(total)

    def one(slot, carry):
        row = coords_ref[0, step * group + slot]
        col = coords_ref[1, step * group + slot]
        at = pl.ds(pl.multiple_of((col % here) * tile, tile), tile)
        source = jnp.concatenate([panel_ref[q, col // here, at, :] for q in range(pairs)], axis=1)
        to = pl.ds(pl.multiple_of(row * tile, tile), tile)
        total[to, :] += jnp.dot(tiles_ref[slot], source, preferred_element_type=jnp.float32)
        return carry

    lax.fori_loop(0, jnp.clip(count - step * group, 0, group), one, 0)

    @pl.when(step == pl.num_programs(0) - 1)
    def _():
        outs = weight.shape[0] // 2
        for h in range(2):
            weight[h * outs:(h + 1) * outs, :] = jnp.concatenate(
                [panel_ref[q, h, nodes:, :] for q in range(pairs)], axis=1
            )
        parts, _, width = out_ref.shape
        block = 256

        def finish(i, carry):
            at = pl.ds(pl.multiple_of(i * block, block), block)
            result = lax.dot_general(
                total[at, :].astype(jnp.bfloat16), weight[...],
                (((1,), (1,)), ((), ())), preferred_element_type=jnp.float32,
            ).astype(out_ref.dtype)
            for d in range(parts):
                out_ref[d, at, :] = result[:, d * width:(d + 1) * width]
            return carry

        lax.fori_loop(0, total.shape[0] // block, finish, 0)


def spread(coords, counts, panel, tiles, outs, parts):
    maxt, tile, _ = tiles.shape
    pairs, _, rows, wide = panel.shape
    nodes = rows - outs // 2
    feat = pairs * wide
    group = min(GROUP, maxt)
    return pl.pallas_call(
        functools.partial(spread_kernel, nodes),
        grid=(maxt // group,),
        out_shape=jax.ShapeDtypeStruct((parts, TROW * tile, outs // parts), jnp.bfloat16),
        in_specs=[
            pl.BlockSpec(memory_space=pltpu.SMEM),
            pl.BlockSpec(memory_space=pltpu.SMEM),
            pl.BlockSpec(memory_space=pltpu.VMEM),
            pl.BlockSpec((group, tile, tile), lambda i: (i, 0, 0)),
        ],
        out_specs=pl.BlockSpec(memory_space=pltpu.VMEM),
        scratch_shapes=[
            pltpu.VMEM((TROW * tile, feat), jnp.float32),
            pltpu.VMEM((outs, feat), jnp.bfloat16),
        ],
        compiler_params=pltpu.CompilerParams(vmem_limit_bytes=VMEM_LIMIT),
        name="spread",
    )(coords, counts, panel, tiles)


def reduce_kernel(parts, part_ref, out_ref, slots, send_sem, recv_sem):
    me = lax.axis_index("col")
    right = lax.rem(me + 1, parts)
    left = lax.rem(me + parts - 1, parts)
    rows = part_ref.shape[1]
    thick = rows // 2 // REDUCE_PIECES

    barrier = pltpu.get_barrier_semaphore()
    for other in (right, left):
        pl.semaphore_signal(
            barrier, inc=1, device_id={"col": other}, device_id_type=pl.DeviceIdType.MESH
        )
    pl.semaphore_wait(barrier, 2)

    def aim(way, step):
        return lax.rem(me + parts - 1 - step, parts) if way == 0 else lax.rem(me + 1 + step, parts)

    def mine(way, step, index):
        return part_ref.at[aim(way, step), pl.ds(way * (rows // 2) + index * thick, thick)]

    def slot(way, step, index):
        return slots.at[way, step, pl.ds(index * thick, thick)]

    def move(way, step, index):
        source = mine(way, 0, index) if step == 0 else slot(way, step - 1, index)
        return remote(source, slot(way, step, index), send_sem.at[way, step, index],
                      recv_sem.at[way, step, index], "col", right if way == 0 else left)

    issued = []
    for index in range(REDUCE_PIECES):
        for way in range(2):
            copy = move(way, 0, index)
            copy.start()
            issued.append(copy)
    held = None
    for step in range(parts - 1):
        for index in range(REDUCE_PIECES):
            for way in range(2):
                move(way, step, index).wait_recv()
                arrived = slot(way, step, index)
                added = (arrived[...].astype(jnp.float32)
                         + mine(way, step + 1, index)[...].astype(jnp.float32)).astype(out_ref.dtype)
                if step < parts - 2:
                    arrived[...] = added
                else:
                    out_ref[pl.ds(way * (rows // 2) + index * thick, thick)] = added
                if held is not None:
                    held.start()
                    issued.append(held)
                    held = None
                if step < parts - 2:
                    held = move(way, step + 1, index)
    for copy in issued:
        copy.wait_send()


def reduce(part):
    parts, rows, width = part.shape
    return pl.pallas_call(
        functools.partial(reduce_kernel, parts),
        out_shape=jax.ShapeDtypeStruct((rows, width), part.dtype),
        in_specs=[pl.BlockSpec(memory_space=pltpu.VMEM)],
        out_specs=pl.BlockSpec(memory_space=pltpu.VMEM),
        scratch_shapes=[
            pltpu.VMEM((2, parts - 1, rows // 2, width), part.dtype),
            pltpu.SemaphoreType.DMA((2, parts - 1, REDUCE_PIECES)),
            pltpu.SemaphoreType.DMA((2, parts - 1, REDUCE_PIECES)),
        ],
        compiler_params=pltpu.CompilerParams(
            collective_id=1, has_side_effects=True, vmem_limit_bytes=VMEM_LIMIT
        ),
        name="reduce",
    )(part)


def solution(mesh):
    placed = (
        P("col", "row"),
        P(None, "row"),
        P(("row", "col"), None, None),
        P(None, ("row", "col")),
        P(("row", "col")),
    )
    pairs = mesh.shape["row"] // 2
    parts = mesh.shape["col"]

    def body(features, weight_t, tiles, coords, counts):
        panel = gather(features, weight_t, pairs)
        part = spread(coords, counts, panel, tiles, weight_t.shape[0], parts)
        return reduce(part)

    return jax.shard_map(
        body, mesh=mesh, in_specs=placed, out_specs=P("row", "col"), check_vma=False
    )
```

```python
import functools

import jax
import jax.numpy as jnp
from jax import lax
from jax.experimental import pallas as pl
from jax.experimental.pallas import tpu as pltpu
from jax.sharding import PartitionSpec as P

TROW = 32
GATHER_PIECES = 8
REDUCE_PIECES = 8
BUNCH = 4
VMEM_LIMIT = 62 * 1024 * 1024


def swapped(p):
    return p + ((p // 2) % 2) * (1 - 2 * (p % 2))


def remote(src, dst, send, recv, axis, to):
    return pltpu.make_async_remote_copy(
        src_ref=src,
        dst_ref=dst,
        send_sem=send,
        recv_sem=recv,
        device_id={axis: to},
        device_id_type=pl.DeviceIdType.MESH,
    )


def gather_kernel(pairs, f_ref, w_ref, panel_ref, half_f, half_w,
                  pre_send, pre_recv, send_sem, recv_sem, sib_send, sib_recv):
    me = lax.axis_index("row")
    core = me % 2
    place = swapped(me // 2)
    sibling = me + 1 - 2 * core
    right = 2 * swapped(lax.rem(place + 1, pairs)) + core
    left = 2 * swapped(lax.rem(place + pairs - 1, pairs)) + core
    nodes = half_f.shape[1]
    outs = half_w.shape[1]
    thick = (nodes + outs) // GATHER_PIECES
    half = GATHER_PIECES // 2

    barrier = pltpu.get_barrier_semaphore()
    for other in (sibling, right, left):
        pl.semaphore_signal(
            barrier, inc=1, device_id={"row": other}, device_id_type=pl.DeviceIdType.MESH
        )
    pl.semaphore_wait(barrier, 3)

    theirs = 1 - core
    pre = [
        remote(f_ref.at[:, pl.ds(pl.multiple_of(theirs * nodes, nodes), nodes)], half_f,
               pre_send.at[0], pre_recv.at[0], "row", sibling),
        remote(w_ref.at[:, pl.ds(pl.multiple_of(theirs * outs, outs), outs)], half_w,
               pre_send.at[1], pre_recv.at[1], "row", sibling),
    ]
    for copy in pre:
        copy.start()
    for copy in pre:
        copy.wait()
    pair = me // 2

    def pack(mine_ref, other_ref, count, base):
        step = min(count, 512)
        for at in range(0, count, step):
            own = mine_ref[:, pl.ds(pl.multiple_of(core * count + at, step), step)]
            other = other_ref[:, at:at + step]
            first = jnp.where(core == 0, own, other)
            second = jnp.where(core == 0, other, own)
            panel_ref[pair, core, base + at:base + at + step] = jnp.concatenate([first, second], axis=0).T

    pack(f_ref, half_f, nodes, 0)
    pack(w_ref, half_w, outs, nodes)

    sends = []

    def piece(position, index):
        return panel_ref.at[swapped(position), core, pl.ds(index * thick, thick)]

    def along(way, distance, position, index, to):
        ref = piece(position, index)
        return remote(ref, ref, send_sem.at[way, distance, index],
                      recv_sem.at[way, distance, index], "row", to)

    sib_at = [0]

    def share(position, index):
        ref = piece(position, index)
        copy = remote(ref, ref, sib_send.at[sib_at[0]], sib_recv.at[sib_at[0]], "row", sibling)
        sib_at[0] += 1
        copy.start()
        sends.append(copy)

    longest = pairs // 2

    def carried(way, distance):
        indices = list(range(GATHER_PIECES)) if way == 0 else list(range(half, GATHER_PIECES)) + list(range(half))
        return indices if distance < longest else indices[:half]

    def start(way, distance, position, index):
        copy = along(way, distance, position, index, right if way == 0 else left)
        copy.start()
        return copy

    issued = []
    for i in range(GATHER_PIECES):
        for way in range(2):
            issued.append(start(way, 0, place, carried(way, 0)[i]))
    for i in range(GATHER_PIECES):
        share(place, i)
    for distance in range(1, longest + 1):
        from_left = lax.rem(place + pairs - distance, pairs)
        from_right = lax.rem(place + distance, pairs)
        for i in range(len(carried(0, distance))):
            for way, position in ((0, from_left), (1, from_right)):
                index = carried(way, distance)[i]
                along(way, distance - 1, position, index, right).wait_recv()
                if distance < longest and index in carried(way, distance + 1):
                    issued.append(start(way, distance, position, index))
                share(position, index)
    for copy in issued:
        copy.wait_send()
    for copy in sends:
        copy.wait()


def gather(features, weight_t, pairs):
    width, nodes = features.shape
    outs = weight_t.shape[1]
    rows = (nodes + outs) // 2
    longest = pairs // 2
    return pl.pallas_call(
        functools.partial(gather_kernel, pairs),
        out_shape=jax.ShapeDtypeStruct((pairs, 2, rows, 2 * width), features.dtype),
        in_specs=[pl.BlockSpec(memory_space=pltpu.VMEM)] * 2,
        out_specs=pl.BlockSpec(memory_space=pltpu.VMEM),
        scratch_shapes=[
            pltpu.VMEM((width, nodes // 2), features.dtype),
            pltpu.VMEM((width, outs // 2), features.dtype),
            pltpu.SemaphoreType.DMA((2,)),
            pltpu.SemaphoreType.DMA((2,)),
            pltpu.SemaphoreType.DMA((2, longest, GATHER_PIECES)),
            pltpu.SemaphoreType.DMA((2, longest, GATHER_PIECES)),
            pltpu.SemaphoreType.DMA((pairs * GATHER_PIECES,)),
            pltpu.SemaphoreType.DMA((pairs * GATHER_PIECES,)),
        ],
        compiler_params=pltpu.CompilerParams(
            collective_id=0, has_side_effects=True, vmem_limit_bytes=VMEM_LIMIT
        ),
        name="gather",
    )(features, weight_t)


def spread_kernel(nodes, coords_ref, counts_ref, panel_hbm, tiles_hbm, out_ref,
                  panel_ref, tiles_ref, total, total_low, weight, listed, where_from, lengths, sems):
    maxt, tile, _ = tiles_hbm.shape
    pairs = panel_ref.shape[0]
    here = nodes // tile
    room = listed.shape[0] // TROW
    count = counts_ref[0]
    copies = [
        pltpu.make_async_copy(panel_hbm, panel_ref, sems.at[0]),
        pltpu.make_async_copy(tiles_hbm, tiles_ref.at[pl.ds(0, maxt)], sems.at[1]),
    ]
    for copy in copies:
        copy.start()

    tiles_ref[maxt] = jnp.zeros((tile, tile), tiles_ref.dtype)

    def clear(row, carry):
        lengths[row] = 0
        return carry

    lax.fori_loop(0, TROW, clear, 0)

    def enter(slot, carry):
        row = coords_ref[0, slot]
        length = lengths[row]
        listed[row * room + length] = slot
        where_from[row * room + length] = coords_ref[1, slot]
        lengths[row] = length + 1
        return carry

    lax.fori_loop(0, count, enter, 0)

    def fill(row, carry):
        for k in range(BUNCH - 1):
            listed[row * room + lengths[row] + k] = maxt
            where_from[row * room + lengths[row] + k] = 0
        return carry

    lax.fori_loop(0, TROW, fill, 0)
    for copy in copies:
        copy.wait()

    outs = weight.shape[0] // 2
    for h in range(2):
        weight[h * outs:(h + 1) * outs, :] = jnp.concatenate(
            [panel_ref[q, h, nodes:, :] for q in range(pairs)], axis=1
        )

    def one_row(row, carry):
        def bunch(i, inner):
            left, right = [], []
            for k in range(BUNCH):
                at = row * room + i * BUNCH + k
                col = where_from[at]
                span = pl.ds(pl.multiple_of((col % here) * tile, tile), tile)
                left.append(tiles_ref[listed[at]])
                right.append(jnp.concatenate(
                    [panel_ref[q, col // here, span, :] for q in range(pairs)], axis=1))
            total[...] += jnp.dot(
                jnp.concatenate(left, axis=1), jnp.concatenate(right, axis=0),
                preferred_element_type=jnp.float32,
            )
            return inner

        total[...] = jnp.zeros_like(total)
        lax.fori_loop(0, (lengths[row] + BUNCH - 1) // BUNCH, bunch, 0)
        total_low[pl.ds(pl.multiple_of(row * tile, tile), tile), :] = total[...].astype(total_low.dtype)
        return carry

    lax.fori_loop(0, TROW, one_row, 0)
    parts, rows, width = out_ref.shape
    block = 512

    def finish(i, carry):
        at = pl.ds(pl.multiple_of(i * block, block), block)
        result = lax.dot_general(
            total_low[at, :], weight[...],
            (((1,), (1,)), ((), ())), preferred_element_type=jnp.float32,
        ).astype(out_ref.dtype)
        for d in range(parts):
            out_ref[d, at, :] = result[:, d * width:(d + 1) * width]
        return carry

    lax.fori_loop(0, rows // block, finish, 0)


def spread(coords, counts, panel, tiles, outs, parts):
    maxt, tile, _ = tiles.shape
    pairs, _, rows, wide = panel.shape
    nodes = rows - outs // 2
    feat = pairs * wide
    room = 2 * nodes // tile + BUNCH
    return pl.pallas_call(
        functools.partial(spread_kernel, nodes),
        out_shape=jax.ShapeDtypeStruct((parts, TROW * tile, outs // parts), jnp.bfloat16),
        in_specs=[
            pl.BlockSpec(memory_space=pltpu.SMEM),
            pl.BlockSpec(memory_space=pltpu.SMEM),
            pl.BlockSpec(memory_space=pl.ANY),
            pl.BlockSpec(memory_space=pl.ANY),
        ],
        out_specs=pl.BlockSpec(memory_space=pltpu.VMEM),
        scratch_shapes=[
            pltpu.VMEM(panel.shape, panel.dtype),
            pltpu.VMEM((maxt + 1, tile, tile), tiles.dtype),
            pltpu.VMEM((tile, feat), jnp.float32),
            pltpu.VMEM((TROW * tile, feat), jnp.bfloat16),
            pltpu.VMEM((outs, feat), jnp.bfloat16),
            pltpu.SMEM((TROW * room,), jnp.int32),
            pltpu.SMEM((TROW * room,), jnp.int32),
            pltpu.SMEM((TROW,), jnp.int32),
            pltpu.SemaphoreType.DMA((2,)),
        ],
        compiler_params=pltpu.CompilerParams(vmem_limit_bytes=VMEM_LIMIT),
        name="spread",
    )(coords, counts, panel, tiles)


def reduce_kernel(parts, part_ref, out_ref, slots, send_sem, recv_sem):
    me = lax.axis_index("col")
    right = lax.rem(me + 1, parts)
    left = lax.rem(me + parts - 1, parts)
    rows = part_ref.shape[1]
    thick = rows // 2 // REDUCE_PIECES

    barrier = pltpu.get_barrier_semaphore()
    for other in (right, left):
        pl.semaphore_signal(
            barrier, inc=1, device_id={"col": other}, device_id_type=pl.DeviceIdType.MESH
        )
    pl.semaphore_wait(barrier, 2)

    def aim(way, step):
        return lax.rem(me + parts - 1 - step, parts) if way == 0 else lax.rem(me + 1 + step, parts)

    def mine(way, step, index):
        return part_ref.at[aim(way, step), pl.ds(way * (rows // 2) + index * thick, thick)]

    def slot(way, step, index):
        return slots.at[way, step, pl.ds(index * thick, thick)]

    def move(way, step, index):
        source = mine(way, 0, index) if step == 0 else slot(way, step - 1, index)
        return remote(source, slot(way, step, index), send_sem.at[way, step, index],
                      recv_sem.at[way, step, index], "col", right if way == 0 else left)

    issued = []
    for index in range(REDUCE_PIECES):
        for way in range(2):
            copy = move(way, 0, index)
            copy.start()
            issued.append(copy)
    held = None
    for step in range(parts - 1):
        for index in range(REDUCE_PIECES):
            for way in range(2):
                move(way, step, index).wait_recv()
                arrived = slot(way, step, index)
                added = (arrived[...].astype(jnp.float32)
                         + mine(way, step + 1, index)[...].astype(jnp.float32)).astype(out_ref.dtype)
                if step < parts - 2:
                    arrived[...] = added
                else:
                    out_ref[pl.ds(way * (rows // 2) + index * thick, thick)] = added
                if held is not None:
                    held.start()
                    issued.append(held)
                    held = None
                if step < parts - 2:
                    held = move(way, step + 1, index)
    for copy in issued:
        copy.wait_send()


def reduce(part):
    parts, rows, width = part.shape
    return pl.pallas_call(
        functools.partial(reduce_kernel, parts),
        out_shape=jax.ShapeDtypeStruct((rows, width), part.dtype),
        in_specs=[pl.BlockSpec(memory_space=pltpu.VMEM)],
        out_specs=pl.BlockSpec(memory_space=pltpu.VMEM),
        scratch_shapes=[
            pltpu.VMEM((2, parts - 1, rows // 2, width), part.dtype),
            pltpu.SemaphoreType.DMA((2, parts - 1, REDUCE_PIECES)),
            pltpu.SemaphoreType.DMA((2, parts - 1, REDUCE_PIECES)),
        ],
        compiler_params=pltpu.CompilerParams(
            collective_id=1, has_side_effects=True, vmem_limit_bytes=VMEM_LIMIT
        ),
        name="reduce",
    )(part)


def solution(mesh):
    placed = (
        P("col", "row"),
        P(None, "row"),
        P(("row", "col"), None, None),
        P(None, ("row", "col")),
        P(("row", "col")),
    )
    pairs = mesh.shape["row"] // 2
    parts = mesh.shape["col"]

    def body(features, weight_t, tiles, coords, counts):
        panel = gather(features.T, weight_t.T, pairs)
        part = spread(coords, counts, panel, tiles, weight_t.shape[0], parts)
        return reduce(part)

    return jax.shard_map(
        body, mesh=mesh, in_specs=placed, out_specs=P("row", "col"), check_vma=False
    )
```
